512 devices in a mesh: groups: 2 (over y), ep: 32 (over z), tp: 4 (over x), sub: 2 (over core).
Axes of the slice: x: 4, y: 2, z: 32, core: 2. Of those that a mesh axis runs over, the one named last changes fastest.
The devices are a block of a 4x8x32 slice.
Arguments:
- queries: bfloat16 [1024, 64, 128], P(('groups', 'ep', 'sub'), 'tp'), parts along dimension 0, may hold values from -80 to 80
- new_keys: bfloat16 [1024, 4, 128], P(('groups', 'ep', 'sub'), 'tp'), parts along dimension 0, may hold values from -4 to 4
- new_values: bfloat16 [1024, 4, 128], P(('groups', 'ep', 'sub'), 'tp'), parts along dimension 0, may hold values from -5 to 5
- key_codes: int32 [1024, 4, 8, 128], P(('groups', 'ep', 'sub'), 'tp'), parts along dimension 0, may hold values from -2147483648 to 2147483647, as said below
- key_scale: bfloat16 [1024, 4, 4, 128], P(('groups', 'ep', 'sub'), 'tp'), parts along dimension 0, may hold values from 0.19921875 to 1
- key_zero: bfloat16 [1024, 4, 4, 128], P(('groups', 'ep', 'sub'), 'tp'), parts along dimension 0, may hold values from -1.5 to 0.5
- value_codes: int32 [1024, 4, 8, 128], P(('groups', 'ep', 'sub'), 'tp'), parts along dimension 0, may hold values from -2147483648 to 2147483647, as said below
- value_scale: bfloat16 [1024, 4, 128], P(('groups', 'ep', 'sub'), 'tp'), parts along dimension 0, may hold values from 0.19921875 to 1
- value_zero: bfloat16 [1024, 4, 128], P(('groups', 'ep', 'sub'), 'tp'), parts along dimension 0, may hold values from -1.1953125 to 0.19921875
- lengths: int32 [1024], P(('groups', 'ep', 'sub')), parts along dimension 0, may hold values from 1 to 128, as said below
- out_weight: bfloat16 [8192, 2048], P('tp', ('ep', 'sub')), may hold values from -0.0625 to 0.0625
- residual: bfloat16 [1024, 2048], P(('groups', 'ep', 'sub'), 'tp'), parts along dimension 0, may hold values from -8 to 8
- norm_gain: bfloat16 [2048], P('tp'), may hold values from 0.099609375 to 1.8984375
- expert_ids: int32 [1024, 8], P(('groups', 'ep', 'sub')), parts along dimension 0, may hold values from 0 to 63, all different within a row; in each aligned block of 8 rows (0 to 7, 8 to 15, ...) at most 2 rows name the same one
- route_weights: int32 [1024, 8], P(('groups', 'ep', 'sub')), parts along dimension 0, may hold values from 1 to 65535
- capacity: int32 [128], P('groups'), parts along dimension 0, may hold values from 16 to 32, as said below
- w_gate: bfloat16 [64, 2048, 768], P(('ep', 'sub'), 'tp'), may hold values from -0.125 to 0.125
- w_up: bfloat16 [64, 2048, 768], P(('ep', 'sub'), 'tp'), may hold values from -0.125 to 0.125
- w_down: bfloat16 [64, 768, 2048], P(('ep', 'sub'), None, 'tp'), may hold values from -0.21875 to 0.21875
Outputs:
- mixed: bfloat16 [1024, 2048], P(('groups', 'ep', 'sub'), 'tp'), parts along dimension 0
The draws below stay inside these ranges and needn't reach their ends.
There are 2 independent parts, one for each index of `groups`. The reference program is written for one: setup_inputs(seed, part) draws one part's arguments, and reference() takes and returns one part's arrays. A program takes and returns all parts, laid end to end along the dimension named above; an argument that names none is the same for every part. Nothing has to cross between parts.
Inputs may be any that keep to these rules, and one draw needn't show every extreme that they name: `key_codes`: each word holds 16 two-bit codes: position 16 w + j in bits 2 j and 2 j + 1 of word w. `value_codes`: packed as key_codes. `lengths`: some request of the batch has exactly 128 cached positions. `expert_ids`: each row names 8 different experts; within the rows of one device (aligned blocks of 8 rows) no expert is named by more than 2 rows, and that bound is reached. Several experts have capacity 32.
All inputs are finite; a program needn't handle non-finite values.
Results may differ from the reference program's by a relative error of at most 0.014.
Values may be sent and summed in bfloat16 or wider, within the bound.
A program may use at most 64 MiB of HBM per device.

```python
import math
import jax
import jax.numpy as jnp
import numpy as np
from jax import lax

D = 2048
FF = 768
HQ = 64
KV = 4
HD = 128
TOP = 8
GROUP = 32
REQ = 8
LMAX = 128
BATCH = 512
EXPERTS = 64
SLOT = 2
CAP = 32


def fresh_keys(key):
    drawn = jax.random.normal(jax.random.fold_in(key, 11), (BATCH, KV, HD), jnp.float32)
    return jnp.clip(drawn, -4.0, 4.0)


def draw_new_keys(key, part):
    return fresh_keys(key).astype(jnp.bfloat16)


def draw_queries(key, part):
    drawn = jnp.clip(jax.random.normal(jax.random.fold_in(key, 12), (BATCH, HQ, HD), jnp.float32), -5.0, 5.0)
    return drawn.astype(jnp.bfloat16)


def packed_codes(key):
    word_shape = (BATCH, KV, LMAX // 16, HD)
    high_half = jax.random.randint(jax.random.fold_in(key, 1), word_shape, 0, 65536, jnp.int32)
    low_half = jax.random.randint(jax.random.fold_in(key, 2), word_shape, 0, 65536, jnp.int32)
    return jnp.bitwise_or(jnp.left_shift(high_half, jnp.int32(16)), low_half).astype(jnp.int32)


def draw_key_codes(key, part):
    return packed_codes(jax.random.fold_in(key, 21))


def draw_value_codes(key, part):
    return packed_codes(jax.random.fold_in(key, 22))


def draw_lengths(key, part):
    drawn = jax.random.randint(jax.random.fold_in(key, 31), (BATCH,), 1, LMAX + 1, jnp.int32)
    full_row = jax.random.randint(jax.random.fold_in(key, 32), (), 0, BATCH, jnp.int32)
    return jnp.where(jnp.arange(BATCH) == full_row, LMAX, drawn).astype(jnp.int32)


def draw_capacity(key, part):
    drawn = jax.random.randint(jax.random.fold_in(key, 51), (EXPERTS,), CAP // 2, CAP + 1, jnp.int32)
    at_most = jax.random.randint(jax.random.fold_in(key, 52), (EXPERTS,), 0, 4, jnp.int32) == 0
    full_one = jax.random.randint(jax.random.fold_in(key, 53), (), 0, EXPERTS, jnp.int32)
    at_most = at_most | (jnp.arange(EXPERTS) == full_one)
    return jnp.where(at_most, CAP, drawn).astype(jnp.int32)


def draw_residual(key, part):
    drawn = 0.5 * jax.random.normal(jax.random.fold_in(key, 41), (BATCH, D), jnp.float32)
    return jnp.clip(drawn, -8.0, 8.0).astype(jnp.bfloat16)


def set_ends(values, stream_key, smallest, largest):
    place = [jax.random.randint(jax.random.fold_in(stream_key, axis), (), 0, length) for axis, length in enumerate(values.shape)]
    longest = values.shape.index(max(values.shape))
    next_to = place[:longest] + [(place[longest] + 1) % values.shape[longest]] + place[longest + 1:]
    return values.at[tuple(place)].set(smallest).at[tuple(next_to)].set(largest)


def block_scale(key, extent, shards, low, top_value):
    gain, own = 1.0, jax.random.fold_in(key, 6)
    for axis_at, blocks in shards:
        steps = jnp.exp(jax.random.uniform(jax.random.fold_in(own, axis_at), (blocks,), jnp.float32, low / len(shards), top_value / len(shards)))
        gain = gain * jnp.repeat(steps, extent[axis_at] // blocks).reshape([-1 if axis == axis_at else 1 for axis in range(len(extent))])
    return gain


def routed_block(own_key, own, number, rows, number_of, top, reach, skew):
    order = jax.random.permutation(own_key, number_of)
    crowded, ordinary = load_shares(number_of, rows * top, reach, skew, True), load_shares(number_of, rows * top, reach, skew, False)
    places = jnp.arange(number_of)

    def named(sizes, offset_by):
        used = int((sizes > 0).sum())
        fixed = max(1, used // 4)
        shifted = fixed + (places - fixed + offset_by * (used - fixed)) % max(1, number_of - fixed)
        return jnp.zeros((number_of,), jnp.int32).at[order[jnp.where(places < fixed, places, shifted)]].set(jnp.asarray(sizes, jnp.int32))

    sizes = jnp.where(number % 4 == 0, named(crowded, number // 4), named(ordinary, number - number // 4 - 1))
    mixed = jax.random.permutation(jax.random.fold_in(own, 3), number_of)
    donor, sink = mixed[0:number_of // 2 * 2:2], mixed[1:number_of // 2 * 2:2]
    slack = jnp.minimum(sizes[donor] - 1, reach - sizes[sink]) // 2
    slack = jnp.where((donor == order[0]) | (sink == order[0]) | (sizes[sink] == 0), 0, jnp.maximum(slack, 0))
    shifted = jax.random.randint(jax.random.fold_in(own, 4), (number_of // 2,), 0, 1 << 20) % (slack + 1)
    sizes = sizes.at[donor].add(-shifted).at[sink].add(shifted)
    items = jnp.searchsorted(jnp.cumsum(sizes), jnp.arange(rows * top), side="right").astype(jnp.int32)
    grid = items.reshape(top, rows).T
    grid = grid[jax.random.permutation(jax.random.fold_in(own, 1), rows)]
    offset_by = jax.random.randint(jax.random.fold_in(own, 2), (rows, 1), 0, top)
    return jnp.take_along_axis(grid, (jnp.arange(top)[None, :] + offset_by) % top, axis=1)


def load_shares(amount, total, limit, skew, full):
    portions = [(1 << 20) // math.isqrt(standing ** skew) + 1 for standing in range(1, amount + 1)]
    largest = limit if full else min(limit, max(-(-total // amount), total * portions[0] // sum(portions)))
    least = 1 if total - largest >= amount - 1 else 0
    given, surplus = [largest] + [least] * (amount - 1), total - largest - least * (amount - 1)
    while surplus > 0:
        candidates = [i for i in range(1, amount) if given[i] < largest] or [i for i in range(1, amount) if given[i] < limit]
        whole, budget = sum([portions[i] for i in candidates]), surplus
        for i in candidates:
            extra = min(limit - given[i], max(1, budget * portions[i] // whole), surplus)
            given[i] = given[i] + extra
            surplus = surplus - extra
    return np.array(given)


def normal_values(rng, dims, spread, reach, shards=(), held_as=jnp.bfloat16):
    gain = block_scale(rng, dims, shards, -0.22, 0.18) if shards else 1.0
    values = jax.random.normal(rng, dims, jnp.float32) * spread * gain
    return jnp.minimum(jnp.maximum(values, -reach), reach).astype(held_as)


def setup_inputs(seed: int = 0, part: int = 0) -> dict:
    key_of = jax.random.split(jax.random.key(seed), 20)
    own_keys = jax.random.split(jax.random.fold_in(key_of[19], part), 20)
    queries = draw_queries(jax.random.fold_in(jax.random.fold_in(key_of[19], part), 71), part)
    new_keys = draw_new_keys(jax.random.fold_in(jax.random.fold_in(key_of[19], part), 71), part)
    new_values = normal_values(own_keys[2], (BATCH, KV, HD), 1.0, 5.0, ((0, 64), (1, 4)))
    key_codes = draw_key_codes(jax.random.fold_in(jax.random.fold_in(key_of[19], part), 71), part)
    key_scale = jnp.clip(0.19921875 + 0.80078125 * jax.random.uniform(own_keys[4], (BATCH, KV, LMAX // GROUP, HD), jnp.float32) ** block_scale(own_keys[4], (BATCH, KV, LMAX // GROUP, HD), ((0, 64), (1, 4)), -0.2, 0.2), 0.19921875, 1.0).astype(jnp.bfloat16)
    key_zero = jnp.clip(-1.5 + 2.0 * jax.random.uniform(own_keys[5], (BATCH, KV, LMAX // GROUP, HD), jnp.float32) ** block_scale(own_keys[5], (BATCH, KV, LMAX // GROUP, HD), ((0, 64), (1, 4)), -0.2, 0.2), -1.5, 0.5).astype(jnp.bfloat16)
    value_codes = draw_value_codes(jax.random.fold_in(jax.random.fold_in(key_of[19], part), 71), part)
    value_scale = jnp.clip(0.19921875 + 0.80078125 * jax.random.uniform(own_keys[7], (BATCH, KV, LMAX), jnp.float32) ** block_scale(own_keys[7], (BATCH, KV, LMAX), ((0, 64), (1, 4)), -0.2, 0.2), 0.19921875, 1.0).astype(jnp.bfloat16)
    value_zero = jnp.clip(-1.1953125 + 1.3945312 * jax.random.uniform(own_keys[8], (BATCH, KV, LMAX), jnp.float32) ** block_scale(own_keys[8], (BATCH, KV, LMAX), ((0, 64), (1, 4)), -0.2, 0.2), -1.1953125, 0.19921875).astype(jnp.bfloat16)
    lengths = draw_lengths(jax.random.fold_in(jax.random.fold_in(key_of[19], part), 71), part)
    out_weight = normal_values(key_of[10], (HQ * HD, D), (HQ * HD) ** -0.5, 0.0625, ((0, 4), (1, 64)))
    residual = draw_residual(jax.random.fold_in(jax.random.fold_in(key_of[19], part), 71), part)
    norm_gain = jnp.clip(1.0 + 0.18 * jax.random.normal(key_of[12], (D,), jnp.float32), 0.099609375, 1.8984375).astype(jnp.bfloat16)
    expert_ids_keys = jax.random.split(jax.random.fold_in(own_keys[13], 1), BATCH // REQ)
    expert_ids_turns = jax.random.permutation(jax.random.fold_in(own_keys[13], 3), BATCH // REQ)
    expert_ids = jax.vmap(lambda own, number: routed_block(jax.random.fold_in(own_keys[13], 2), own, number, REQ, EXPERTS, TOP, SLOT, 2))(expert_ids_keys, expert_ids_turns).reshape((BATCH, TOP))
    route_weights = set_ends(jax.random.randint(own_keys[14], (BATCH, TOP), 1, 65536), jax.random.fold_in(own_keys[14], 1), 1, 65535).astype(jnp.int32)
    capacity = draw_capacity(jax.random.fold_in(jax.random.fold_in(key_of[19], part), 71), part)
    w_gate = normal_values(key_of[16], (EXPERTS, D, FF), D ** -0.5, 0.125, ((0, 64), (1, 4)))
    w_up = normal_values(key_of[17], (EXPERTS, D, FF), D ** -0.5, 0.125, ((0, 64), (1, 4)))
    w_down = normal_values(key_of[18], (EXPERTS, FF, D), FF ** -0.5, 0.21875, ((0, 64), (2, 4)))
    return {"queries": queries, "new_keys": new_keys, "new_values": new_values, "key_codes": key_codes, "key_scale": key_scale, "key_zero": key_zero, "value_codes": value_codes, "value_scale": value_scale, "value_zero": value_zero, "lengths": lengths, "out_weight": out_weight, "residual": residual, "norm_gain": norm_gain, "expert_ids": expert_ids, "route_weights": route_weights, "capacity": capacity, "w_gate": w_gate, "w_up": w_up, "w_down": w_down}


EPS = 1e-06

def unpack_codes(packed_words):
    shifts = (2 * jnp.arange(16)).astype(jnp.int32)
    code_vals = jnp.bitwise_and(jnp.right_shift(packed_words[..., None, :], shifts[:, None]), 3)
    word_shape = packed_words.shape
    return code_vals.reshape(word_shape[:-2] + (word_shape[-2] * 16, word_shape[-1])).astype(jnp.float32)

def attend_one(request_data):
    query_heads, key_new, value_new, key_words, key_step, key_offset, value_words, value_step, value_offset, seq_length = request_data
    kv_heads, head_dim = key_new.shape
    token_group = key_words.shape[1] * 16 // key_step.shape[1]
    keys_deq = unpack_codes(key_words) * jnp.repeat(key_step.astype(jnp.float32), token_group, axis=1)
    keys_deq = (keys_deq + jnp.repeat(key_offset.astype(jnp.float32), token_group, axis=1)).astype(jnp.bfloat16)
    values_deq = unpack_codes(value_words) * value_step.astype(jnp.float32)[:, :, None] + value_offset.astype(jnp.float32)[:, :, None]
    values_deq = values_deq.astype(jnp.bfloat16)
    grouped = query_heads.reshape(kv_heads, -1, head_dim).astype(jnp.float32)
    inv_scale = 1.0 / math.sqrt(head_dim)
    scores = jnp.einsum('kgd,kld->kgl', grouped, keys_deq.astype(jnp.float32)) * inv_scale
    own_score = jnp.einsum('kgd,kd->kg', grouped, key_new.astype(jnp.float32)) * inv_scale
    usable = jnp.arange(keys_deq.shape[1]) < seq_length
    scores = jnp.where(usable, scores, -jnp.inf)
    highest = jnp.maximum(lax.optimization_barrier(jnp.max(scores, axis=2)), own_score)
    weights = jnp.exp(scores - highest[:, :, None])
    own_weight = jnp.exp(own_score - highest)
    totals = lax.optimization_barrier(jnp.sum(weights, axis=2)) + own_weight
    weights = (weights / totals[:, :, None]).astype(jnp.bfloat16)
    own_weight = (own_weight / totals).astype(jnp.bfloat16)
    result = jnp.einsum('kgl,kld->kgd', weights.astype(jnp.float32), values_deq.astype(jnp.float32))
    result = result + own_weight.astype(jnp.float32)[:, :, None] * value_new.astype(jnp.float32)[:, None, :]
    return result.reshape(-1).astype(jnp.bfloat16)

def reference(queries, new_keys, new_values, key_codes, key_scale, key_zero, value_codes, value_scale, value_zero, lengths, out_weight, residual, norm_gain, expert_ids, route_weights, capacity, w_gate, w_up, w_down):
    attended = lax.map(attend_one, (queries, new_keys, new_values, key_codes, key_scale, key_zero, value_codes, value_scale, value_zero, lengths))
    projected = jnp.dot(attended, out_weight, preferred_element_type=jnp.float32)
    hidden_state = residual.astype(jnp.float32) + projected
    mean_square = lax.optimization_barrier(jnp.mean(hidden_state * hidden_state, axis=1, keepdims=True))
    normed = (hidden_state * lax.rsqrt(mean_square + EPS) * norm_gain.astype(jnp.float32)).astype(jnp.bfloat16)
    raw_weight = route_weights.astype(jnp.float32)
    shares = raw_weight / lax.optimization_barrier(jnp.sum(raw_weight, axis=1, keepdims=True))
    experts_all = w_gate.shape[0]
    chosen = (expert_ids[:, :, None] == jnp.arange(experts_all).astype(jnp.int32)).astype(jnp.int32)
    is_named = lax.optimization_barrier(jnp.sum(chosen, axis=1)).astype(jnp.int32)
    rank = (jnp.cumsum(is_named, axis=0) - is_named).astype(jnp.int32)
    kept = is_named * (rank < capacity[None, :]).astype(jnp.int32)
    weight_per = lax.optimization_barrier(jnp.sum(chosen.astype(jnp.float32) * shares[:, :, None], axis=1)) * kept.astype(jnp.float32)
    slot_ids = jnp.arange(CAP).astype(jnp.int32)

    def one_expert(totals, per_expert):
        keep_col, rank_col, weight_col, gate_w, up_w, down_w = per_expert
        packer = ((rank_col[None, :] == slot_ids[:, None]) & (keep_col[None, :] > 0)).astype(jnp.bfloat16)
        packed_rows = jnp.dot(packer, normed, preferred_element_type=jnp.float32).astype(jnp.bfloat16)
        gate_sum = jnp.dot(packed_rows, gate_w, preferred_element_type=jnp.float32)
        up_sum = jnp.dot(packed_rows, up_w, preferred_element_type=jnp.float32)
        activated = (jax.nn.silu(gate_sum) * up_sum).astype(jnp.bfloat16)
        expert_out = jnp.dot(activated, down_w, preferred_element_type=jnp.float32).astype(jnp.bfloat16)
        spread_back = jnp.dot(packer.T, expert_out, preferred_element_type=jnp.float32)
        return (totals + weight_col[:, None] * spread_back, None)
    moe, _ = lax.scan(one_expert, jnp.zeros(hidden_state.shape, jnp.float32), (kept.T, rank.T, weight_per.T, w_gate, w_up, w_down))
    return (hidden_state + moe).astype(jnp.bfloat16)
```

```python
import functools
import math

import jax
import jax.numpy as jnp
from jax import lax
from jax.experimental import pallas as pl
from jax.experimental.pallas import tpu as pltpu
from jax.sharding import PartitionSpec as P

EPS = 1e-06
PIECES = 4
SLOTS = 2
RANKS = 32
MESH = pl.DeviceIdType.MESH
F32, BF16, I32 = jnp.float32, jnp.bfloat16, jnp.int32


def nt_dot(a, b):
    return lax.dot_general(a, b, (((1,), (1,)), ((), ())), preferred_element_type=F32)


def nn_dot(a, b):
    return jnp.dot(a, b, preferred_element_type=F32)


def kernel(
    q_ref, nk_ref, nv_ref, kc_ref, ks_ref, kz_ref, vc_ref, vs_ref, vz_ref, len_ref,
    w_ref, res_ref, gain_ref, ids_ref, rw_ref, cap_ref, wg_hbm, wu_hbm, wd_hbm,
    out_ref,
    blocks, counts, att, att_rows, att_both, att_bf, row_f32, proj, rs_send, rs_recv,
    pick_t, comb_t, place, d_send, d_recv, r_send, r_recv,
    wg, wu, wd, g_send, g_recv, act,
    own_sem, w_sem, ring_send, ring_recv, cnt_send, cnt_recv,
    att_sem, cpair_sem, rs_sem, dd_sem, rr_sem, gg_sem, aa_sem,
):
    nz, ntp, nc = lax.axis_size("ep"), lax.axis_size("tp"), lax.axis_size("sub")
    z, tp, sub = lax.axis_index("ep"), lax.axis_index("tp"), lax.axis_index("sub")
    nr = nz * nc
    me = z * nc + sub
    half = nz // 2
    up, down = lax.rem(z + 1, nz), lax.rem(z + nz - 1, nz)
    other = 1 - sub
    ngrp = ntp * nc
    mine = tp * nc + sub
    reqs, heads, hd = q_ref.shape
    cols = blocks.shape[2]
    rows_w = w_ref.shape[1]
    piece = rows_w // PIECES
    quarter = res_ref.shape[1]
    lt = quarter // 128
    msg = SLOTS * lt
    lanes = nr * msg
    inv_scale = 1.0 / math.sqrt(hd)

    own_copies = [
        pltpu.make_async_copy(
            w_ref.at[:, pl.ds(p * piece, piece)], blocks.at[z, p], own_sem.at[p]
        )
        for p in range(PIECES)
    ]
    w_copies = [
        pltpu.make_async_copy(src, dst, w_sem.at[i])
        for i, (src, dst) in enumerate(((wg_hbm, wg), (wu_hbm, wu), (wd_hbm, wd)))
    ]
    for copy in own_copies:
        copy.start()

    barrier = pltpu.get_barrier_semaphore()
    for near in (up, down):
        pl.semaphore_signal(barrier, 1, device_id={"ep": near}, device_id_type=MESH)

    def group_member(k):
        there = lax.rem(mine + k, ngrp)
        return there // nc, lax.rem(there, nc)

    for k in range(1, ngrp):
        there_tp, there_sub = group_member(k)
        pl.semaphore_signal(
            barrier, 1, device_id={"tp": there_tp, "sub": there_sub}, device_id_type=MESH
        )

    ids = ids_ref[...]
    lane128 = lax.broadcasted_iota(I32, (reqs, 128), 1)
    named = jnp.zeros((reqs, 128), F32)
    for k in range(ids.shape[1]):
        named = named + (ids[:, k : k + 1] == lane128).astype(F32)
    counts[sub, z] = jnp.sum(named, axis=0, keepdims=True)

    pl.semaphore_wait(barrier, 2 + ngrp - 1)

    def block_copy(way, step, p):
        at = lax.rem(z - step + nz, nz) if way == 0 else lax.rem(z + step, nz)
        return pltpu.make_async_remote_copy(
            src_ref=blocks.at[at, p],
            dst_ref=blocks.at[at, p],
            send_sem=ring_send.at[way, step, p],
            recv_sem=ring_recv.at[way, step, p],
            device_id={"ep": up if way == 0 else down},
            device_id_type=MESH,
        )

    def count_copy(way, step):
        at = lax.rem(z - step + nz, nz) if way == 0 else lax.rem(z + step, nz)
        return pltpu.make_async_remote_copy(
            src_ref=counts.at[sub, at],
            dst_ref=counts.at[sub, at],
            send_sem=cnt_send.at[way, step],
            recv_sem=cnt_recv.at[way, step],
            device_id={"ep": up if way == 0 else down},
            device_id_type=MESH,
        )

    for p in range(PIECES):
        own_copies[p].wait()
        for way in (0, 1):
            block_copy(way, 0, p).start()
    for way in (0, 1):
        count_copy(way, 0).start()
    for copy in w_copies:
        copy.start()

    def pass_on(step, p):
        for way in (0, 1):
            block_copy(way, step - 1, p).wait_recv()
            block_copy(way, step, p).start()

    def pass_counts(step):
        for way in (0, 1):
            count_copy(way, step - 1).wait_recv()
            count_copy(way, step).start()

    def attend_scores(b):
        sixteen = 2 * lax.broadcasted_iota(I32, (16, hd), 0)
        words = kc_ref[b]
        steps = ks_ref[b].astype(F32)
        zeros = kz_ref[b].astype(F32)
        per_group = words.shape[0] // steps.shape[0]
        keys = []
        for w in range(words.shape[0]):
            codes = jnp.bitwise_and(jnp.right_shift(words[w : w + 1, :], sixteen), 3)
            g = w // per_group
            keys.append(codes.astype(F32) * steps[g : g + 1, :] + zeros[g : g + 1, :])
        keys = jnp.concatenate(keys, axis=0).astype(BF16)
        q = q_ref[b]
        scores = nt_dot(q, keys) * inv_scale
        own = jnp.sum(q.astype(F32) * row_f32[0, b], axis=1, keepdims=True) * inv_scale
        usable = lax.broadcasted_iota(I32, scores.shape, 1) < len_ref[b]
        scores = jnp.where(usable, scores, -jnp.inf)
        highest = jnp.maximum(jnp.max(scores, axis=1, keepdims=True), own)
        weights = jnp.exp(scores - highest)
        own = jnp.exp(own - highest)
        totals = jnp.sum(weights, axis=1, keepdims=True) + own
        att[b, 0] = (weights / totals).astype(BF16).astype(F32)
        att[b, 1] = jnp.broadcast_to((own / totals).astype(BF16).astype(F32), (heads, hd))

    def attend_values(b):
        sixteen = 2 * lax.broadcasted_iota(I32, (16, hd), 0)
        words = vc_ref[b]
        values = []
        for w in range(words.shape[0]):
            codes = jnp.bitwise_and(jnp.right_shift(words[w : w + 1, :], sixteen), 3)
            values.append(codes.astype(F32))
        values = jnp.concatenate(values, axis=0).astype(BF16)
        weights = att[b, 0]
        scaled = weights * row_f32[2, b]
        high = scaled.astype(BF16)
        low = (scaled - high.astype(F32)).astype(BF16)
        summed = nn_dot(jnp.concatenate([high, low], axis=0), values)
        offset = jnp.sum(weights * row_f32[3, b], axis=1, keepdims=True)
        result = summed[:heads] + summed[heads:] + offset + att[b, 1] * row_f32[1, b]
        att_rows[pl.ds(pl.multiple_of(b * heads, heads), heads), :] = result.astype(BF16).astype(F32)

    for i, ref in enumerate((nk_ref, nv_ref, vs_ref, vz_ref)):
        rows = ref[...].astype(F32)
        for b in range(reqs):
            row_f32[i, b] = rows[b : b + 1, :]

    n_att = max(1, half // 4)
    per_step = reqs // n_att

    def attention_step(step, _):
        first = (step - 1) * per_step
        for p in range(PIECES):
            pass_on(step, p)
            if p == 0:
                pass_counts(step)
                for b in range((per_step + 1) // 2):
                    attend_scores(first + b)
            elif p == 1:
                for b in range((per_step + 1) // 2, per_step):
                    attend_scores(first + b)
            elif p == 2:
                for b in range((per_step + 1) // 2):
                    attend_values(first + b)
            else:
                for b in range((per_step + 1) // 2, per_step):
                    attend_values(first + b)
        return 0

    lax.fori_loop(1, n_att + 1, attention_step, 0)

    for h in range(heads):
        att_both[sub, :, h * hd : (h + 1) * hd] = att_rows[pl.ds(h, reqs, stride=heads), :]
    att_copy = pltpu.make_async_remote_copy(
        src_ref=att_both.at[sub],
        dst_ref=att_both.at[sub],
        send_sem=att_sem.at[0],
        recv_sem=att_sem.at[1],
        device_id={"sub": other},
        device_id_type=MESH,
    )
    att_copy.start()

    lane = lax.broadcasted_iota(I32, (reqs, lanes), 1)
    expert_at = lane // msg
    slot_at = lax.rem(lane, msg) // lt
    tile_at = lax.rem(lane, lt)
    raw = rw_ref[...].astype(F32)
    shares = raw / jnp.sum(raw, axis=1, keepdims=True)
    named = jnp.zeros((reqs, lanes), F32)
    weight = jnp.zeros((reqs, lanes), F32)
    for k in range(ids.shape[1]):
        hit = ids[:, k : k + 1] == expert_at
        named = jnp.where(hit, 1.0, named)
        weight = jnp.where(hit, shares[:, k : k + 1], weight)
    running = jnp.zeros((1, lanes), F32)
    ranks = []
    for b in range(reqs):
        ranks.append(running)
        running = running + named[b : b + 1, :]
    local_rank = jnp.concatenate(ranks, axis=0)
    chosen = jnp.where(local_rank == slot_at.astype(F32), named, 0.0)
    weight = weight * chosen
    high = weight.astype(BF16).astype(F32)
    low = weight - high
    for l in range(lt):
        here = tile_at == l
        pick_t[l * reqs : (l + 1) * reqs, :] = jnp.where(here, chosen, 0.0)
        comb_t[l * reqs : (l + 1) * reqs, :] = jnp.where(here, high, 0.0).astype(BF16)
        comb_t[(lt + l) * reqs : (lt + l + 1) * reqs, :] = jnp.where(here, low, 0.0).astype(BF16)
    pick = jnp.transpose(pick_t[...]).astype(BF16)

    att_copy.wait()
    both = att_both[...].reshape(nc * reqs, rows_w)
    att_bf[...] = both.astype(BF16)

    def project(at):
        total = nt_dot(att_bf[:, 0:piece], blocks[at, 0])
        for p in range(1, PIECES):
            total += nt_dot(att_bf[:, p * piece : (p + 1) * piece], blocks[at, p])
        proj[at] = total

    def behind(distance):
        return lax.rem(z - distance + nz, nz)

    def ahead(distance):
        return lax.rem(z + distance, nz)

    def catch_up_step(step, _):
        for p in range(PIECES):
            pass_on(step, p)
            if p == 0:
                pass_counts(step)
                project(behind(step - 1 - n_att))
            elif p == 1:
                project(ahead(step - 1 - n_att))
            elif p == 2:
                project(behind(step - 1))
            else:
                project(ahead(step - 1))
        return 0

    def projection_step(step, _):
        for p in range(PIECES):
            pass_on(step, p)
            if p == 0:
                pass_counts(step)
            elif p == 1:
                project(behind(step - 1))
            elif p == 2:
                project(ahead(step - 1))
        return 0

    lax.fori_loop(n_att + 1, 2 * n_att + 1, catch_up_step, 0)
    lax.fori_loop(2 * n_att + 1, half - 1, projection_step, 0)

    last = half - 1
    for p in range(PIECES):
        for way in (0, 1):
            block_copy(way, last - 1, p).wait_recv()
            if (p < PIECES // 2) == (way == 0):
                block_copy(way, last, p).start()
        if p == 0:
            for way in (0, 1):
                count_copy(way, last - 1).wait_recv()
            count_copy(0, last).start()
        elif p == 1:
            project(behind(last - 1))
        elif p == 2:
            project(ahead(last - 1))
    project(behind(last))
    project(ahead(last))
    count_copy(0, last).wait_recv()
    count_pair = pltpu.make_async_remote_copy(
        src_ref=counts.at[sub],
        dst_ref=counts.at[sub],
        send_sem=cpair_sem.at[0],
        recv_sem=cpair_sem.at[1],
        device_id={"sub": other},
        device_id_type=MESH,
    )
    count_pair.start()
    for p in range(PIECES):
        block_copy(0 if p < PIECES // 2 else 1, last, p).wait_recv()
    project(ahead(half))

    per_quarter = nz // ntp
    for t in range(ntp):
        part = jnp.concatenate([proj[t * per_quarter + i] for i in range(per_quarter)], axis=1)
        for c in range(nc):
            rs_send[t * nc + c] = part[c * reqs : (c + 1) * reqs, :].astype(BF16)

    def rs_copy(k):
        there_tp, there_sub = group_member(k)
        return pltpu.make_async_remote_copy(
            src_ref=rs_send.at[lax.rem(mine + k, ngrp)],
            dst_ref=rs_recv.at[k - 1],
            send_sem=rs_sem.at[0, k],
            recv_sem=rs_sem.at[1, k],
            device_id={"tp": there_tp, "sub": there_sub},
            device_id_type=MESH,
        )

    for k in range(1, ngrp):
        rs_copy(k).start()
    sums = [rs_send[mine].astype(F32), None]
    for k in range(1, ngrp):
        rs_copy(k).wait_recv()
        got = rs_recv[k - 1].astype(F32)
        side = k % nc
        sums[side] = got if sums[side] is None else sums[side] + got
    own_first = sub == 0
    first = jnp.where(own_first, sums[0], sums[1])
    second = jnp.where(own_first, sums[1], sums[0])
    hidden = jnp.concatenate(
        [
            side[:, i * cols : (i + 1) * cols]
            for i in range(per_quarter)
            for side in (first, second)
        ],
        axis=1,
    ) + res_ref[...].astype(F32)

    hidden_bf = hidden.astype(BF16)
    stacked = jnp.concatenate([hidden_bf[:, l * 128 : (l + 1) * 128].astype(F32) for l in range(lt)], axis=0)
    outgoing = nn_dot(pick, stacked.astype(BF16)).astype(BF16)
    d_send[...] = outgoing.reshape(nr, msg, 128)

    def far_first(i):
        return nr // 2 + ((i + 1) // 2) * (2 * lax.rem(i, 2) - 1)

    def d_copy(k):
        there = lax.rem(me + k, nr)
        return pltpu.make_async_remote_copy(
            src_ref=d_send.at[there],
            dst_ref=d_recv.at[k - 1],
            send_sem=dd_sem.at[0],
            recv_sem=dd_sem.at[1],
            device_id={"ep": there // nc, "sub": lax.rem(there, nc)},
            device_id_type=MESH,
        )

    count_pair.wait()

    def d_start(i, _):
        d_copy(far_first(i)).start()
        return 0

    lax.fori_loop(0, nr - 1, d_start, 0)
    d_recv[nr - 1] = d_send[me]

    one_lane = (lax.broadcasted_iota(I32, (8, 128), 1) == me).astype(BF16)
    cnt_rows = [counts[c].reshape(nz, 128).astype(BF16) for c in range(nc)]
    cnt8 = [nt_dot(one_lane, rows).astype(BF16) for rows in cnt_rows]
    col = lax.broadcasted_iota(I32, (nz, lanes), 1)
    source = lax.rem(me + 2 * nr - 1 - col // msg, nr)
    row_z = lax.broadcasted_iota(I32, (nz, lanes), 0)
    before = jnp.zeros((8, lanes), F32)
    here = jnp.zeros((8, lanes), F32)
    for c in range(nc):
        row_id = row_z * nc + c
        before = before + nn_dot(cnt8[c], (row_id < source).astype(F32).astype(BF16))
        here = here + nn_dot(cnt8[c], (row_id == source).astype(F32).astype(BF16))
    lane1 = lax.broadcasted_iota(I32, (1, lanes), 1)
    slot1 = (lax.rem(lane1, msg) // lt).astype(F32)
    tile1 = lax.rem(lane1, lt)
    position = before[0:1] + slot1
    valid = (slot1 < here[0:1]) & (position < cap_ref[me].astype(F32))
    position = jnp.where(valid, position, -1.0)
    rank_at = lax.broadcasted_iota(I32, (RANKS, lanes), 0).astype(F32)
    for l in range(lt):
        hit = (rank_at == position) & (tile1 == l)
        place[l * RANKS : (l + 1) * RANKS, :] = jnp.where(hit, 1.0, 0.0)
    place_bf = place[...].astype(BF16)
    spread_bf = jnp.transpose(place[...]).astype(BF16)
    for copy in w_copies:
        copy.wait()

    pltpu.make_async_copy(d_recv.at[pl.ds(0, nr - 1)], d_recv.at[pl.ds(0, nr - 1)], dd_sem.at[1]).wait()

    packed = nn_dot(place_bf, d_recv[...].reshape(lanes, 128))
    packed = jnp.concatenate([packed[l * RANKS : (l + 1) * RANKS] for l in range(lt)], axis=1)
    squares = jnp.sum(packed * packed, axis=1, keepdims=True)
    gained = (packed * gain_ref[...].astype(F32)).astype(BF16)
    ff = wg.shape[1]
    own_rows = RANKS // ntp
    gate = nn_dot(gained, wg[...])
    upper = nn_dot(gained, wu[...])
    sq_high = squares.astype(BF16).astype(F32)
    on_left = lax.broadcasted_iota(I32, (RANKS, 128), 1) < 64
    sq_both = jnp.where(on_left, sq_high, squares - sq_high)
    for t in range(ntp):
        span = slice(t * own_rows, (t + 1) * own_rows)
        g_send[t, :, 0:ff] = gate[span].astype(BF16)
        g_send[t, :, ff : 2 * ff] = upper[span].astype(BF16)
        g_send[t, :, 2 * ff :] = sq_both[span].astype(BF16)

    def g_copy(k):
        there = lax.rem(tp + k, ntp)
        return pltpu.make_async_remote_copy(
            src_ref=g_send.at[there],
            dst_ref=g_recv.at[k - 1],
            send_sem=gg_sem.at[0, k],
            recv_sem=gg_sem.at[1, k],
            device_id={"tp": there},
            device_id_type=MESH,
        )

    far_tp = sorted(range(1, ntp), key=lambda k: -min(k, ntp - k))
    for k in far_tp:
        g_copy(k).start()
    total = g_send[tp].astype(F32)
    for k in range(1, ntp):
        g_copy(k).wait_recv()
        total = total + g_recv[k - 1].astype(F32)
    square = total[:, 2 * ff : 2 * ff + 1] + total[:, 2 * ff + 64 : 2 * ff + 65]
    scale = lax.rsqrt(square / (quarter * ntp) + EPS)
    gate = total[:, 0:ff] * scale
    upper = total[:, ff : 2 * ff] * scale
    act[tp] = (gate / (1.0 + jnp.exp(-gate)) * upper).astype(BF16)

    def a_copy(k):
        return pltpu.make_async_remote_copy(
            src_ref=act.at[tp],
            dst_ref=act.at[tp],
            send_sem=aa_sem.at[0, k],
            recv_sem=aa_sem.at[1, k],
            device_id={"tp": lax.rem(tp + k, ntp)},
            device_id_type=MESH,
        )

    for k in far_tp:
        a_copy(k).start()
    for k in range(1, ntp):
        a_copy(k).wait_recv()
    activated = jnp.concatenate([act[t].astype(F32) for t in range(ntp)], axis=0).astype(BF16)
    result = nn_dot(activated, wd[...])
    stacked = jnp.concatenate([result[:, l * 128 : (l + 1) * 128] for l in range(lt)], axis=0)
    back = nn_dot(spread_bf, stacked.astype(BF16)).astype(BF16)
    r_send[...] = back.reshape(nr, msg, 128)

    def r_copy(k):
        there = lax.rem(me + nr - k, nr)
        return pltpu.make_async_remote_copy(
            src_ref=r_send.at[k - 1],
            dst_ref=r_recv.at[me],
            send_sem=rr_sem.at[0],
            recv_sem=rr_sem.at[1],
            device_id={"ep": there // nc, "sub": lax.rem(there, nc)},
            device_id_type=MESH,
        )

    def r_start(i, _):
        r_copy(far_first(i)).start()
        return 0

    lax.fori_loop(0, nr - 1, r_start, 0)
    r_recv[me] = r_send[nr - 1]

    def sent(step, _):
        for way in (0, 1):
            for p in range(PIECES):
                block_copy(way, step, p).wait_send()
            count_copy(way, step).wait_send()
        return 0

    lax.fori_loop(0, last, sent, 0)
    for p in range(PIECES):
        block_copy(0 if p < PIECES // 2 else 1, last, p).wait_send()
    count_copy(0, last).wait_send()
    for k in range(1, ngrp):
        rs_copy(k).wait_send()
    for k in range(1, ntp):
        g_copy(k).wait_send()
        a_copy(k).wait_send()
    pltpu.make_async_copy(d_recv.at[pl.ds(0, nr - 1)], d_recv.at[pl.ds(0, nr - 1)], dd_sem.at[0]).wait()

    pltpu.make_async_copy(r_recv.at[pl.ds(0, nr - 1)], r_recv.at[pl.ds(0, nr - 1)], rr_sem.at[1]).wait()
    moe = nn_dot(comb_t[...], r_recv[...].reshape(lanes, 128))
    moe = moe[: lt * reqs] + moe[lt * reqs :]
    moe = jnp.concatenate([moe[l * reqs : (l + 1) * reqs] for l in range(lt)], axis=1)
    out_ref[...] = (hidden + moe).astype(BF16)
    pltpu.make_async_copy(r_send.at[pl.ds(0, nr - 1)], r_send.at[pl.ds(0, nr - 1)], rr_sem.at[0]).wait()


def shards(
    queries, new_keys, new_values, key_codes, key_scale, key_zero, value_codes,
    value_scale, value_zero, lengths, out_weight, residual, norm_gain, expert_ids,
    route_weights, capacity, w_gate, w_up, w_down,
):
    nz, ntp, nc = lax.axis_size("ep"), lax.axis_size("tp"), lax.axis_size("sub")
    nr = nz * nc
    reqs, heads, hd = queries.shape
    rows_w, cols = out_weight.shape
    quarter = residual.shape[1]
    channels, ff = w_gate.shape[1:]
    lt = quarter // 128
    msg = SLOTS * lt
    lanes = nr * msg
    half = nz // 2
    ngrp = ntp * nc
    vmem = pl.BlockSpec(memory_space=pltpu.VMEM)
    smem = pl.BlockSpec(memory_space=pltpu.SMEM)
    hbm = pl.BlockSpec(memory_space=pl.ANY)
    dma = pltpu.SemaphoreType.DMA
    return pl.pallas_call(
        kernel,
        out_shape=jax.ShapeDtypeStruct((reqs, quarter), BF16),
        in_specs=[vmem] * 9 + [smem, hbm] + [vmem] * 4 + [smem] + [hbm] * 3,
        out_specs=vmem,
        scratch_shapes=[
            pltpu.VMEM((nz, PIECES, cols, rows_w // PIECES), BF16),
            pltpu.VMEM((nc, nz, 1, 128), F32),
            pltpu.VMEM((reqs, 2, heads, hd), F32),
            pltpu.VMEM((reqs * heads, hd), F32),
            pltpu.VMEM((nc, reqs, rows_w), F32),
            pltpu.VMEM((nc * reqs, rows_w), BF16),
            pltpu.VMEM((4, reqs, 1, hd), F32),
            pltpu.VMEM((nz, nc * reqs, cols), F32),
            pltpu.VMEM((ngrp, reqs, quarter // nc), BF16),
            pltpu.VMEM((ngrp - 1, reqs, quarter // nc), BF16),
            pltpu.VMEM((lt * reqs, lanes), F32),
            pltpu.VMEM((2 * lt * reqs, lanes), BF16),
            pltpu.VMEM((lt * RANKS, lanes), F32),
            pltpu.VMEM((nr, msg, 128), BF16),
            pltpu.VMEM((nr, msg, 128), BF16),
            pltpu.VMEM((nr, msg, 128), BF16),
            pltpu.VMEM((nr, msg, 128), BF16),
            pltpu.VMEM((channels, ff), BF16),
            pltpu.VMEM((channels, ff), BF16),
            pltpu.VMEM((ff, quarter), BF16),
            pltpu.VMEM((ntp, RANKS // ntp, 2 * ff + 128), BF16),
            pltpu.VMEM((max(1, ntp - 1), RANKS // ntp, 2 * ff + 128), BF16),
            pltpu.VMEM((ntp, RANKS // ntp, ff), BF16),
            dma((PIECES,)),
            dma((3,)),
            dma((2, half, PIECES)),
            dma((2, half, PIECES)),
            dma((2, half)),
            dma((2, half)),
            dma((2,)),
            dma((2,)),
            dma((2, ngrp)),
            dma((2,)),
            dma((2,)),
            dma((2, ntp)),
            dma((2, ntp)),
        ],
        compiler_params=pltpu.CompilerParams(collective_id=0, has_side_effects=True),
        name="decode_moe",
    )(
        queries,
        new_keys.reshape(reqs, hd),
        new_values.reshape(reqs, hd),
        key_codes.reshape(reqs, -1, hd),
        key_scale.reshape(reqs, -1, hd),
        key_zero.reshape(reqs, -1, hd),
        value_codes.reshape(reqs, -1, hd),
        value_scale.reshape(reqs, -1),
        value_zero.reshape(reqs, -1),
        lengths,
        out_weight.T,
        residual,
        norm_gain.reshape(1, quarter),
        expert_ids,
        route_weights,
        capacity,
        w_gate.reshape(channels, ff),
        w_up.reshape(channels, ff),
        w_down.reshape(ff, quarter),
    )


def solution(mesh):
    return jax.shard_map(
        shards,
        mesh=mesh,
        in_specs=(
            P(("groups", "ep", "sub"), "tp", None),
            P(("groups", "ep", "sub"), "tp", None),
            P(("groups", "ep", "sub"), "tp", None),
            P(("groups", "ep", "sub"), "tp", None, None),
            P(("groups", "ep", "sub"), "tp", None, None),
            P(("groups", "ep", "sub"), "tp", None, None),
            P(("groups", "ep", "sub"), "tp", None, None),
            P(("groups", "ep", "sub"), "tp", None),
            P(("groups", "ep", "sub"), "tp", None),
            P(("groups", "ep", "sub")),
            P("tp", ("ep", "sub")),
            P(("groups", "ep", "sub"), "tp"),
            P("tp"),
            P(("groups", "ep", "sub"), None),
            P(("groups", "ep", "sub"), None),
            P("groups"),
            P(("ep", "sub"), "tp", None),
            P(("ep", "sub"), "tp", None),
            P(("ep", "sub"), None, "tp"),
        ),
        out_specs=P(("groups", "ep", "sub"), "tp"),
        check_vma=False,
    )
```
